128 devices in a mesh: third: 4 (over z), second: 4 (over y), group: 8 (over x, core).
Axes of the slice: x: 4, y: 4, z: 4, core: 2. Of those that a mesh axis runs over, the one named last changes fastest.
Arguments:
- x_one: bfloat16 [16384, 2048], P(('third', 'second', 'group'))
- z_one: bfloat16 [16384, 8192], P(('third', 'second', 'group'))
- x_two: bfloat16 [16384, 2048], P(('third', 'second', 'group'))
- z_two: bfloat16 [16384, 8192], P(('third', 'second', 'group'))
- grad_out: bfloat16 [16384, 2048], P(('third', 'second', 'group'))
- w1_in: bfloat16 [2048, 8192], replicated
- w1_out: bfloat16 [8192, 2048], replicated
- w2_in: bfloat16 [2048, 8192], replicated
- w2_out: bfloat16 [8192, 2048], replicated
Outputs:
- output 1: float32 [8192, 2048], replicated
- output 2: float32 [2048, 8192], replicated
- output 3: float32 [8192, 2048], replicated
- output 4: float32 [2048, 8192], replicated
- output 5: bfloat16 [16384, 2048], P(('third', 'second', 'group'))
All inputs are finite; a program needn't handle non-finite values.
Results may differ from the reference program's by a relative error of at most 0.00524652.
Values are sent between devices in bfloat16 or wider.
A program may use at most 1.5 GiB of HBM per device.

```python
import math
import jax
import jax.numpy as jnp
from jax import lax

D = 2048
FF = 8192
TOKENS = 128
DEVICES = 128

INV_ROOT_TWO = math.sqrt(0.5)
INV_ROOT_TWO_PI = 1.0 / math.sqrt(2.0 * math.pi)


def gelu_pair(z_pre):
    z_val = z_pre.astype(jnp.float32)
    cdf_val = 0.5 * (1.0 + lax.erf(z_val * INV_ROOT_TWO))
    hidden = (z_val * cdf_val).astype(jnp.bfloat16)
    slope = cdf_val + z_val * jnp.exp(-0.5 * z_val * z_val) * INV_ROOT_TWO_PI
    return hidden, slope


def block_backward(x_in, z_pre, grad_y, w_in, w_out):
    hidden, slope = gelu_pair(z_pre)
    w_out_grad = jnp.dot(hidden.T, grad_y, preferred_element_type=jnp.float32).astype(jnp.bfloat16)
    grad_hidden = jnp.dot(grad_y, w_out.T, preferred_element_type=jnp.float32)
    grad_pre = (grad_hidden * slope).astype(jnp.bfloat16)
    w_in_grad = jnp.dot(x_in.T, grad_pre, preferred_element_type=jnp.float32).astype(jnp.bfloat16)
    grad_x = (grad_y.astype(jnp.float32) + jnp.dot(grad_pre, w_in.T, preferred_element_type=jnp.float32)).astype(jnp.bfloat16)
    return w_out_grad, w_in_grad, grad_x


def setup_inputs(seed: int = 0) -> dict:
    keys = jax.random.split(jax.random.key(seed), 9)
    row_count = DEVICES * TOKENS

    def normal_draw(key_part, shape_in, factor):
        return (jax.random.normal(key_part, shape_in, jnp.float32) * factor).astype(jnp.bfloat16)

    return dict(
        x_one=normal_draw(keys[0], (row_count, D), 1.0),
        z_one=normal_draw(keys[1], (row_count, FF), 1.0),
        x_two=normal_draw(keys[2], (row_count, D), 1.0),
        z_two=normal_draw(keys[3], (row_count, FF), 1.0),
        grad_out=normal_draw(keys[4], (row_count, D), row_count ** -0.25),
        w1_in=normal_draw(keys[5], (D, FF), D ** -0.5),
        w1_out=normal_draw(keys[6], (FF, D), FF ** -0.5),
        w2_in=normal_draw(keys[7], (D, FF), D ** -0.5),
        w2_out=normal_draw(keys[8], (FF, D), FF ** -0.5),
    )


def reference(x_one, z_one, x_two, z_two, grad_out, w1_in, w1_out, w2_in, w2_out):
    def by_device(arr):
        return arr.reshape(DEVICES, TOKENS, arr.shape[-1])

    def device_step(run_sums, batch):
        x_one_dev, z_one_dev, x_two_dev, z_two_dev, grad_dev = batch
        w2o_grad, w2i_grad, dx_two = block_backward(x_two_dev, z_two_dev, grad_dev, w2_in, w2_out)
        w1o_grad, w1i_grad, dx_one = block_backward(x_one_dev, z_one_dev, dx_two, w1_in, w1_out)
        new_sums = tuple(run_sum + grad_part.astype(jnp.float32) for run_sum, grad_part in zip(run_sums, (w2o_grad, w2i_grad, w1o_grad, w1i_grad)))
        return new_sums, dx_one

    zero_sums = (
        jnp.zeros((FF, D), jnp.float32),
        jnp.zeros((D, FF), jnp.float32),
        jnp.zeros((FF, D), jnp.float32),
        jnp.zeros((D, FF), jnp.float32),
    )
    batches = (by_device(x_one), by_device(z_one), by_device(x_two), by_device(z_two), by_device(grad_out))
    total_sums, grad_rows = lax.scan(device_step, zero_sums, batches)
    return (total_sums[0], total_sums[1], total_sums[2], total_sums[3], grad_rows.reshape(DEVICES * TOKENS, D))
```

```python
import functools
import math
import jax
import jax.numpy as jnp
from jax import lax
from jax.experimental import pallas as pl
from jax.experimental.pallas import tpu as pltpu
from jax.sharding import PartitionSpec as P

AXES = ('third', 'second', 'group')
INV_ROOT_TWO = math.sqrt(0.5)
INV_ROOT_TWO_PI = 1.0 / math.sqrt(2.0 * math.pi)
CONTRACT_ROWS = (((0,), (0,)), ((), ()))
CONTRACT_COLS = (((1,), (1,)), ((), ()))


def gelu_pair(z_pre):
    z_val = z_pre.astype(jnp.float32)
    cdf_val = 0.5 * (1.0 + lax.erf(z_val * INV_ROOT_TWO))
    hidden = (z_val * cdf_val).astype(jnp.bfloat16)
    slope = cdf_val + z_val * jnp.exp(-0.5 * z_val * z_val) * INV_ROOT_TWO_PI
    return hidden, slope


def block_factors(z_pre, grad_y, w_in, w_out):
    hidden, slope = gelu_pair(z_pre)
    grad_hidden = lax.dot_general(grad_y, w_out, CONTRACT_COLS, preferred_element_type=jnp.float32)
    grad_pre = (grad_hidden * slope).astype(jnp.bfloat16)
    grad_x = (grad_y.astype(jnp.float32) + lax.dot_general(grad_pre, w_in, CONTRACT_COLS, preferred_element_type=jnp.float32)).astype(jnp.bfloat16)
    return hidden, grad_pre, grad_x


def rounded_sum(lhs_ref, rhs_ref, lhs_cols, rhs_cols):
    total = None
    for dev in range(lhs_ref.shape[0]):
        prod = lax.dot_general(lhs_ref[dev, :, lhs_cols], rhs_ref[dev, :, rhs_cols], CONTRACT_ROWS, preferred_element_type=jnp.float32)
        prod = prod.astype(jnp.bfloat16).astype(jnp.float32)
        total = prod if total is None else total + prod
    return total


def out_kernel(wide_ref, narrow_ref, part_ref):
    def body(step, carry):
        rows = pl.ds(pl.multiple_of(step * 128, 128), 128)
        tile = rounded_sum(wide_ref, narrow_ref, rows, slice(None))
        part_ref[pl.ds(step * 2, 2), 0] = tile.reshape(2, 64, tile.shape[-1])
        return carry
    lax.fori_loop(0, wide_ref.shape[-1] // 128, body, 0)


def in_kernel(narrow_ref, wide_ref, part_ref):
    part_ref[...] = rounded_sum(narrow_ref, wide_ref, slice(None), slice(None))


def partial_out(wide, narrow):
    devs, rows, width = wide.shape
    tile = 256
    per = 1024 // tile
    return pl.pallas_call(
        out_kernel,
        grid=(2 * per,),
        in_specs=[pl.BlockSpec((devs, rows, width), lambda i: (0, 0, 0)),
                  pl.BlockSpec((devs, rows, tile), lambda i: (0, 0, i))],
        out_specs=pl.BlockSpec((16, 1, 64, tile), lambda i: (0, i // per, 0, i % per)),
        out_shape=jax.ShapeDtypeStruct((16, 2, 64, 1024), jnp.float32),
        cost_estimate=pl.CostEstimate(flops=2 * devs * rows * width * 2048, bytes_accessed=16 << 20, transcendentals=0),
        name='partial_out',
    )(wide, narrow).reshape(2048, 1024)


def partial_in(narrow, wide):
    devs, rows, width = wide.shape
    tile = 128
    return pl.pallas_call(
        in_kernel,
        grid=(2048 // tile,),
        in_specs=[pl.BlockSpec((devs, rows, tile), lambda i: (0, 0, i)),
                  pl.BlockSpec((devs, rows, width), lambda i: (0, 0, 0))],
        out_specs=pl.BlockSpec((tile, width), lambda i: (i, 0)),
        out_shape=jax.ShapeDtypeStruct((2048, 1024), jnp.float32),
        cost_estimate=pl.CostEstimate(flops=2 * devs * rows * width * 2048, bytes_accessed=16 << 20, transcendentals=0),
        name='partial_in',
    )(narrow, wide)


def place_out_kernel(in_ref, out_ref):
    for g in range(8):
        out_ref[g, 0, :, :1024] = in_ref[0, g, 0, :64, :]
        out_ref[g, 0, :, 1024:] = in_ref[0, g, 0, 64:, :]


def place_in_kernel(in_ref, out_ref):
    for g in range(8):
        out_ref[:, g * 1024:(g + 1) * 1024] = in_ref[0, g, 0]


def place(gathered, index, transposed):
    cost = pl.CostEstimate(flops=1 << 30, bytes_accessed=128 << 20, transcendentals=0)
    in_spec = pl.BlockSpec((1, 8, 1, 128, 1024), lambda i: (i, 0, index, 0, 0))
    if transposed:
        return pl.pallas_call(
            place_in_kernel, grid=(16,), in_specs=[in_spec],
            out_specs=pl.BlockSpec((128, 8192), lambda i: (i, 0)),
            out_shape=jax.ShapeDtypeStruct((2048, 8192), jnp.float32),
            cost_estimate=cost, name='place_in',
        )(gathered)
    return pl.pallas_call(
        place_out_kernel, grid=(16,), in_specs=[in_spec],
        out_specs=pl.BlockSpec((8, 1, 64, 2048), lambda i: (0, i, 0, 0)),
        out_shape=jax.ShapeDtypeStruct((8, 16, 64, 2048), jnp.float32),
        cost_estimate=cost, name='place_out',
    )(gathered).reshape(8192, 2048)


def exchange_wide(arr):
    rows, cols = arr.shape
    return lax.all_to_all(arr.reshape(rows, 8, cols // 8).transpose(1, 0, 2), 'group', 0, 0)


def solution(mesh):
    def device_step(x_one, z_one, x_two, z_two, grad_out, w1_in, w1_out, w2_in, w2_out):
        hid_two, dz_two, dx_two = block_factors(z_two, grad_out, w2_in, w2_out)
        hid_one, dz_one, dx_one = block_factors(z_one, dx_two, w1_in, w1_out)
        narrow = lax.all_gather(jnp.concatenate([grad_out, x_two, x_one], axis=1), 'group', axis=0)
        dy_two_all, x_two_all, x_one_all = narrow[..., :2048], narrow[..., 2048:4096], narrow[..., 4096:]
        dx_two_all = lax.all_gather(dx_two, 'group', axis=0)
        parts = [
            partial_out(exchange_wide(hid_two), dy_two_all),
            partial_in(x_two_all, exchange_wide(dz_two)),
            partial_out(exchange_wide(hid_one), dx_two_all),
            partial_in(x_one_all, exchange_wide(dz_one)),
        ]
        def gather(mine):
            whole = lax.all_gather(mine, AXES, axis=0)
            return whole.reshape(16, 8, mine.shape[0], 128, 1024)

        def rs(part):
            return lax.psum_scatter(part, ('third', 'second'), scatter_dimension=0, tiled=True)
        mine = [rs(part) for part in parts]
        first = gather(jnp.stack(mine[1:]))
        held, first = lax.optimization_barrier((mine[0], first))
        last = gather(held[None])
        return (place(last, 0, False), place(first, 0, True), place(first, 1, False), place(first, 2, True), dx_one)

    row_spec = P(AXES, None)
    repl_spec = P()
    return jax.shard_map(
        device_step, mesh=mesh,
        in_specs=(row_spec,) * 5 + (repl_spec,) * 4,
        out_specs=(repl_spec,) * 4 + (row_spec,),
        check_vma=False,
    )
```

```python
import functools
import math
import jax
import jax.numpy as jnp
from jax import lax
from jax.experimental import pallas as pl
from jax.experimental.pallas import tpu as pltpu
from jax.sharding import PartitionSpec as P

AXES = ('third', 'second', 'group')
MESH = pl.DeviceIdType.MESH
INV_ROOT_TWO = math.sqrt(0.5)
INV_ROOT_TWO_PI = 1.0 / math.sqrt(2.0 * math.pi)
CONTRACT_ROWS = (((0,), (0,)), ((), ()))
CONTRACT_COLS = (((1,), (1,)), ((), ()))
ROLES = (('x', 'y', 'z'), ('y', 'z', 'x'), ('z', 'x', 'y'), ('x', 'y', 'z'))
HALF = 512
CHIPS = 4
LINE = 8
TOKENS = 128
WIDTH = 1024
NARROW = 2048
WIDE = 8192
BOTH = (0, 1)
SLOTS = 6
ORDER = tuple(zip(map(int, '0102130451023410652317647523647523467567'), map(int, '0010102002311134012240121233232344433444')))


def gelu(z_pre):
    z_val = z_pre.astype(jnp.float32)
    return (z_val * (0.5 * (1.0 + lax.erf(z_val * INV_ROOT_TWO)))).astype(jnp.bfloat16)


def slope_of(z_pre):
    z_val = z_pre.astype(jnp.float32)
    cdf_val = 0.5 * (1.0 + lax.erf(z_val * INV_ROOT_TWO))
    return cdf_val + z_val * jnp.exp(-0.5 * z_val * z_val) * INV_ROOT_TWO_PI


def reduce_kernel(hid_two, hid_one, z_two, z_one, grad_out, x_two, x_one, w2_out, w2_in, w1_out,
                  early_ref, late_ref, dz_out, dx_two, land_w, land_n,
                  stage_w, stage_n, part, got1, got2, got3, got4, dz_buf, dy_buf, dx_buf, z_buf,
                  xs_n, xr_n, xs_w, xr_w, stage_sem_w, stage_sem_n, rs_send, rs_recv, z_sem, put_sem):
    narrows = (grad_out, x_two, dx_two, x_one)

    def wide_piece(m, line, h):
        if m % 2:
            return dz_out.at[m // 2, 2 * line + h]
        return (hid_two, hid_one)[m // 2].at[:, pl.ds(pl.multiple_of(line * WIDTH + h * HALF, HALF), HALF)]

    def fetch_tile(which, t):
        slot = t % 2
        if which == 1:
            def columns(k, carry):
                pltpu.make_async_copy(w2_in.at[pl.ds(2 * t, 2), :, pl.ds(pl.multiple_of(k * NARROW, NARROW), NARROW)],
                                      stage_n.at[slot, pl.ds(2 * k, 2)], stage_sem_n.at[slot]).start()
                return carry
            lax.fori_loop(0, 4, columns, 0)
        else:
            pltpu.make_async_copy((w2_out, None, w1_out)[which].at[pl.ds(8 * t, 8)], stage_n.at[slot], stage_sem_n.at[slot]).start()
            z_pre = (z_two, None, z_one)[which]
            pltpu.make_async_copy(z_pre.at[:, pl.ds(pl.multiple_of(t * WIDTH, WIDTH), WIDTH)], z_buf.at[slot], z_sem.at[slot]).start()

    def tiles(which, body):
        def step(t, carry):
            slot = t % 2
            pltpu.make_async_copy(stage_n.at[slot], stage_n.at[slot], stage_sem_n.at[slot]).wait()
            if which != 1:
                pltpu.make_async_copy(z_buf.at[slot], z_buf.at[slot], z_sem.at[slot]).wait()
            body(t, slot)

            @pl.when(t < 6)
            def _():
                fetch_tile(which, t + 2)
            if which < 2:
                @pl.when(t >= 6)
                def _():
                    fetch_tile(which + 1, t - 6)
            return carry
        lax.fori_loop(0, 8, step, 0)

    def weights(slot, pair):
        return stage_n[slot, 2 * pair:2 * pair + 2].reshape(256, NARROW)

    def grad_pre(which, grad_ref):
        def body(t, slot):
            for pair in range(4):
                grad_hidden = lax.dot_general(grad_ref[...], weights(slot, pair), CONTRACT_COLS, preferred_element_type=jnp.float32)
                at = 256 * (pair % 2)
                slope = slope_of(z_buf[slot, :, 256 * pair:256 * pair + 256])
                dz_buf[2 * t + pair // 2, :, at:at + 256] = (grad_hidden * slope).astype(jnp.bfloat16)
        tiles(which, body)
        put = pltpu.make_async_copy(dz_buf, dz_out.at[which // 2], put_sem.at[0])
        put.start()
        put.wait()

    def grad_input():
        def body(t, slot):
            total = None
            for k in range(16):
                at = HALF * (k % CHIPS)
                prod = lax.dot_general(dz_buf[k], weights(slot, k // 4)[:, at:at + HALF], CONTRACT_COLS, preferred_element_type=jnp.float32)
                total = prod if total is None else total + prod
            cols = pl.ds(pl.multiple_of(t * 256, 256), 256)
            dx_buf[:, cols] = (dy_buf[:, cols].astype(jnp.float32) + total).astype(jnp.bfloat16)
        tiles(1, body)
        put = pltpu.make_async_copy(dx_buf, dx_two, put_sem.at[1])
        put.start()
        put.wait()

    fetch_tile(0, 0)
    fetch_tile(0, 1)
    get_dy = pltpu.make_async_copy(grad_out, dy_buf, put_sem.at[1])
    get_dy.start()
    z, y, g = lax.axis_index('third'), lax.axis_index('second'), lax.axis_index('group')
    x, c = g // 2, g % 2
    pos = {'x': x, 'y': y, 'z': z}

    def device(axis, off, core):
        at = dict(pos)
        at[axis] = (pos[axis] + off) % CHIPS
        return (at['z'], at['y'], 2 * at['x'] + core)

    barrier = pltpu.get_barrier_semaphore()
    peers = [device(axis, off, core) for axis in 'xyz' for off in (1, 2, 3) for core in BOTH] + [device('x', 0, 1 - c)]
    for peer in peers:
        pl.semaphore_signal(barrier, inc=1, device_id=peer, device_id_type=MESH)
    pl.semaphore_wait(barrier, len(peers))

    def line_index(m):
        return 2 * pos[ROLES[m][0]] + c

    def direct_narrow(m, off, core):
        return pltpu.make_async_remote_copy(
            src_ref=narrows[m], dst_ref=land_n.at[m, line_index(m)], send_sem=xs_n.at[m, off], recv_sem=xr_n.at[m, line_index(m)],
            device_id=device(ROLES[m][0], off, core), device_id_type=MESH)

    def relay_narrow(m, off):
        source = 2 * ((pos[ROLES[m][0]] + off) % CHIPS) + c
        return pltpu.make_async_remote_copy(
            src_ref=land_n.at[m, source], dst_ref=land_n.at[m, source], send_sem=xs_n.at[m, 3 + off], recv_sem=xr_n.at[m, source],
            device_id=device('x', 0, 1 - c), device_id_type=MESH)

    def wide_copy(m, h, off, core):
        me = line_index(m)
        target = 2 * ((pos[ROLES[m][0]] + off) % CHIPS) + core
        return pltpu.make_async_remote_copy(
            src_ref=wide_piece(m, target, h), dst_ref=land_w.at[m, h, me], send_sem=xs_w.at[m, h, 2 * off + core], recv_sem=xr_w.at[m, h, me],
            device_id=device(ROLES[m][0], off, core), device_id_type=MESH)

    def over_chips(fn):
        lax.fori_loop(1, 4, lambda off, carry: (fn(off), carry)[1], 0)

    def start_narrow(m):
        over_chips(lambda off: direct_narrow(m, off, c).start())
        direct_narrow(m, 0, 1 - c).start()

    def start_wide(m, h):
        def both(off):
            wide_copy(m, h, off, 0).start()
            wide_copy(m, h, off, 1).start()
        over_chips(both)
        wide_copy(m, h, 0, 1 - c).start()

    def relay(m):
        def one(off):
            source = 2 * ((pos[ROLES[m][0]] + off) % CHIPS) + c
            pltpu.make_async_copy(land_n.at[m, source], land_n.at[m, source], xr_n.at[m, source]).wait()
            relay_narrow(m, off).start()
        over_chips(one)

    def wait_exchange_sends(m):
        over_chips(lambda off: direct_narrow(m, off, c).wait_send())
        direct_narrow(m, 0, 1 - c).wait_send()
        over_chips(lambda off: relay_narrow(m, off).wait_send())
        for h in BOTH:
            def both(off):
                wide_copy(m, h, off, 0).wait_send()
                wide_copy(m, h, off, 1).wait_send()
            over_chips(both)
            wide_copy(m, h, 0, 1 - c).wait_send()

    def stage_narrow(m):
        me = line_index(m)
        slot = m % 2

        def other_core(off, carry):
            source = 2 * ((pos[ROLES[m][0]] + off) % CHIPS) + 1 - c
            pltpu.make_async_copy(land_n.at[m, source], land_n.at[m, source], xr_n.at[m, source]).wait()
            return carry
        lax.fori_loop(0, 4, other_core, 0)

        def fetch(off, carry):
            source = (me + off) % LINE
            pltpu.make_async_copy(land_n.at[m, source], stage_n.at[slot, source], stage_sem_n.at[slot]).start()
            return carry
        lax.fori_loop(1, LINE, fetch, 0)
        pltpu.make_async_copy(narrows[m], stage_n.at[slot, me], stage_sem_n.at[slot]).start()

    def stage_wide(m, h):
        me = line_index(m)

        def fetch(off, carry):
            source = (me + off) % LINE
            pltpu.make_async_copy(land_w.at[m, h, source], land_w.at[m, h, source], xr_w.at[m, h, source]).wait()
            pltpu.make_async_copy(land_w.at[m, h, source], stage_w.at[h, source], stage_sem_w.at[h]).start()
            return carry
        lax.fori_loop(1, LINE, fetch, 0)
        pltpu.make_async_copy(wide_piece(m, me, h), stage_w.at[h, me], stage_sem_w.at[h]).start()

    def rs_copy(j, color, stage, side):
        m, h = j // 2, j % 2
        first, second = ROLES[m][1:] if color == 0 else ROLES[m][:0:-1]
        p, q = pos[first], pos[second]
        slot, got = j % SLOTS, j % 6
        sign = 1 if side == 0 else 3
        mine = part.at[slot, color]
        if stage == 1:
            src, dst, axis = mine.at[(p + 2) % CHIPS, pl.ds(2 * side, 2)], got1.at[got, color, side], first
        elif stage == 2:
            src, dst, axis = mine.at[(p + sign) % CHIPS], got2.at[got, color, side], first
        elif stage == 3:
            src, dst, axis = mine.at[p, (q + 2) % CHIPS, pl.ds(32 * side, 32)], got3.at[got, color, side], second
        else:
            src, dst, axis = mine.at[p, (q + sign) % CHIPS], got4.at[got, color, side], second
        return pltpu.make_async_remote_copy(
            src_ref=src, dst_ref=dst, send_sem=rs_send.at[j, color, stage - 1, side], recv_sem=rs_recv.at[j, color, stage - 1, side],
            device_id=device(axis, sign, c), device_id_type=MESH)

    def compute(j):
        m, h = j // 2, j % 2
        slot = j % SLOTS
        a, b = pos[ROLES[m][1]], pos[ROLES[m][2]]
        if h == 0:
            pltpu.make_async_copy(stage_n.at[m % 2], stage_n.at[m % 2], stage_sem_n.at[m % 2]).wait()
        pltpu.make_async_copy(stage_w.at[h], stage_w.at[h], stage_sem_w.at[h]).wait()
        wide, narrow = stage_w.at[h], stage_n.at[m % 2]

        def piece(i, carry):
            k = jnp.maximum(i - 7, 0)
            pa = jnp.where(i < 4, a + 2, jnp.where(i < 7, a + i - 1, a + 3 + k // 3)) % CHIPS
            pb = jnp.where(i < 4, i, jnp.where(i < 7, b + 2, b + 3 + k % 3)) % CHIPS
            if m % 2 == 0:
                lhs, lhs_at, rhs, rhs_at = wide, pa * TOKENS, narrow, pb * HALF
            else:
                lhs, lhs_at, rhs, rhs_at = narrow, (pa * 4 + pb) * TOKENS, wide, 0
            lhs_cols = pl.ds(pl.multiple_of(lhs_at, TOKENS), TOKENS)
            rhs_cols = pl.ds(pl.multiple_of(rhs_at, HALF), HALF) if m % 2 == 0 else slice(None)
            total = None
            for dev in range(8):
                prod = lax.dot_general(lhs[dev, :, lhs_cols], rhs[dev, :, rhs_cols], CONTRACT_ROWS, preferred_element_type=jnp.float32)
                prod = prod.astype(jnp.bfloat16).astype(jnp.float32)
                total = prod if total is None else total + prod
            part[slot, 0, pa, pb] = total[:64]
            part[slot, 1, pb, pa] = total[64:]

            @pl.when(i == 3)
            def _():
                rs_copy(j, 0, 1, 0).start()
                rs_copy(j, 0, 1, 1).start()

            @pl.when(i == 6)
            def _():
                rs_copy(j, 1, 1, 0).start()
                rs_copy(j, 1, 1, 1).start()
            return carry
        lax.fori_loop(0, 16, piece, 0)

    def coords(j, color):
        m = j // 2
        first, second = ROLES[m][1:] if color == 0 else ROLES[m][:0:-1]
        return pos[first], pos[second]

    def stage_two(j):
        slot, got = j % SLOTS, j % 6
        for color in BOTH:
            p, q = coords(j, color)
            rs_copy(j, color, 1, 0).wait_recv()
            part[slot, color, (p + 1) % CHIPS, 0:2] += got1[got, color, 0]
            rs_copy(j, color, 1, 1).wait_recv()
            part[slot, color, (p + 3) % CHIPS, 2:4] += got1[got, color, 1]
            rs_copy(j, color, 2, 0).start()
            rs_copy(j, color, 2, 1).start()

    def stage_three(j):
        slot, got = j % SLOTS, j % 6
        for color in BOTH:
            p, q = coords(j, color)
            rs_copy(j, color, 2, 0).wait_recv()
            rs_copy(j, color, 2, 1).wait_recv()
            part[slot, color, p] += got2[got, color, 0] + got2[got, color, 1]
        for color in BOTH:
            rs_copy(j, color, 3, 0).start()
            rs_copy(j, color, 3, 1).start()

    def stage_four(j):
        slot, got = j % SLOTS, j % 6
        for color in BOTH:
            p, q = coords(j, color)
            rs_copy(j, color, 3, 0).wait_recv()
            part[slot, color, p, (q + 1) % CHIPS, 0:32] += got3[got, color, 0]
            rs_copy(j, color, 3, 1).wait_recv()
            part[slot, color, p, (q + 3) % CHIPS, 32:64] += got3[got, color, 1]
            rs_copy(j, color, 4, 0).start()
            rs_copy(j, color, 4, 1).start()

    def stage_five(j):
        m, h = j // 2, j % 2
        slot, got = j % SLOTS, j % 6
        for color in BOTH:
            p, q = coords(j, color)
            rs_copy(j, color, 4, 0).wait_recv()
            rs_copy(j, color, 4, 1).wait_recv()
            out_ref = late_ref.at[0] if m == 3 else early_ref.at[m]
            out_ref[64 * color:64 * color + 64, h * HALF:(h + 1) * HALF] = part[slot, color, p, q] + got4[got, color, 0] + got4[got, color, 1]

    def drain(j):
        for color in BOTH:
            for stage in (1, 2, 3, 4):
                for side in BOTH:
                    rs_copy(j, color, stage, side).wait_send()

    start_narrow(0)
    start_narrow(1)
    for h in BOTH:
        start_wide(0, h)
    for h in BOTH:
        start_wide(2, h)
    start_narrow(3)
    get_dy.wait()
    grad_pre(0, dy_buf)
    for h in BOTH:
        start_wide(1, h)
    grad_input()
    start_narrow(2)
    relay(0)
    relay(1)
    grad_pre(2, dx_buf)
    for h in BOTH:
        start_wide(3, h)
    stage_narrow(0)
    stage_wide(0, 0)

    def compute_step(j):
        if j == 6:
            relay(3)
            stage_narrow(3)
            stage_wide(3, 0)
        if j >= SLOTS:
            drain(j - SLOTS)
        if j + 1 < 8 and j + 1 != 6:
            if j + 1 == 4:
                relay(2)
            if (j + 1) % 2 == 0:
                stage_narrow((j + 1) // 2)
            stage_wide((j + 1) // 2, (j + 1) % 2)
        compute(j)

    steps = (compute_step, stage_two, stage_three, stage_four, stage_five)
    for job, stage in ORDER:
        steps[stage](job)
    for j in range(8 - SLOTS, 8):
        drain(j)
    for m in range(4):
        wait_exchange_sends(m)


def reduce_factors(*operands):
    f32, bf16, dma = jnp.float32, jnp.bfloat16, pltpu.SemaphoreType.DMA
    any_spec = pl.BlockSpec(memory_space=pl.ANY)
    vmem_spec = pl.BlockSpec(memory_space=pltpu.VMEM)
    return pl.pallas_call(
        reduce_kernel,
        out_shape=(jax.ShapeDtypeStruct((3, TOKENS, WIDTH), f32), jax.ShapeDtypeStruct((1, TOKENS, WIDTH), f32),
                   jax.ShapeDtypeStruct((2, 16, TOKENS, HALF), bf16), jax.ShapeDtypeStruct((TOKENS, NARROW), bf16),
                   jax.ShapeDtypeStruct((4, 2, 8, TOKENS, HALF), bf16), jax.ShapeDtypeStruct((4, 8, TOKENS, NARROW), bf16)),
        in_specs=[any_spec] * len(operands),
        out_specs=(vmem_spec, vmem_spec) + (any_spec,) * 4,
        scratch_shapes=[
            pltpu.VMEM((2, 8, TOKENS, HALF), bf16), pltpu.VMEM((2, 8, TOKENS, NARROW), bf16),
            pltpu.VMEM((SLOTS, 2, 4, 4, 64, HALF), f32),
            pltpu.VMEM((6, 2, 2, 2, 64, HALF), f32), pltpu.VMEM((6, 2, 2, 4, 64, HALF), f32),
            pltpu.VMEM((6, 2, 2, 32, HALF), f32), pltpu.VMEM((6, 2, 2, 64, HALF), f32),
            pltpu.VMEM((16, TOKENS, HALF), bf16), pltpu.VMEM((TOKENS, NARROW), bf16), pltpu.VMEM((TOKENS, NARROW), bf16), pltpu.VMEM((2, TOKENS, WIDTH), bf16),
            dma((4, 8)), dma((4, 8)), dma((4, 2, 8)), dma((4, 2, 8)), dma((2,)), dma((2,)),
            dma((8, 2, 4, 2)), dma((8, 2, 4, 2)), dma((2,)), dma((2,)),
        ],
        compiler_params=pltpu.CompilerParams(collective_id=0, has_side_effects=True, vmem_limit_bytes=67043328),
        cost_estimate=pl.CostEstimate(flops=1 << 34, bytes_accessed=64 << 20, transcendentals=0),
        name='reduce_factors',
    )(*operands)[:4]


def place_out_kernel(lead, in_ref, out_ref):
    for q in range(4):
        for core in BOTH:
            for h in BOTH:
                piece = in_ref[q, 0, 0, core, 0] if lead else in_ref[0, q, 0, core, 0]
                out_ref[core, h, 0, :, q * HALF:(q + 1) * HALF] = piece[:, h * HALF:(h + 1) * HALF]


def place_in_kernel(lead, in_ref, out_ref):
    for e in range(4):
        for core in BOTH:
            at = (2 * e + core) * WIDTH
            out_ref[:, at:at + WIDTH] = in_ref[0, e, 0, core, 0] if lead else in_ref[0, 0, e, core, 0]


def place(gathered, index, m):
    common = dict(grid=(4, 4), name='place', cost_estimate=pl.CostEstimate(flops=1 << 30, bytes_accessed=TOKENS << 20, transcendentals=0))
    f32 = jnp.float32
    if m == 0:
        return pl.pallas_call(
            functools.partial(place_out_kernel, True),
            in_specs=[pl.BlockSpec((4, 1, 1, 2, 1, TOKENS, WIDTH), lambda i, k: (0, i, k, 0, index, 0, 0))],
            out_specs=pl.BlockSpec((2, 2, 1, TOKENS, NARROW), lambda i, k: (k, 0, i, 0, 0)),
            out_shape=jax.ShapeDtypeStruct((8, 2, 4, TOKENS, NARROW), f32), **common)(gathered).reshape(WIDE, NARROW)
    if m == 2:
        return pl.pallas_call(
            functools.partial(place_out_kernel, False),
            in_specs=[pl.BlockSpec((1, 4, 1, 2, 1, TOKENS, WIDTH), lambda i, k: (k, 0, i, 0, index, 0, 0))],
            out_specs=pl.BlockSpec((2, 2, 1, TOKENS, NARROW), lambda i, k: (k, 0, i, 0, 0)),
            out_shape=jax.ShapeDtypeStruct((8, 2, 4, TOKENS, NARROW), f32), **common)(gathered).reshape(WIDE, NARROW)
    if m == 1:
        return pl.pallas_call(
            functools.partial(place_in_kernel, True),
            in_specs=[pl.BlockSpec((1, 4, 1, 2, 1, TOKENS, WIDTH), lambda i, k: (i, 0, k, 0, index, 0, 0))],
            out_specs=pl.BlockSpec((TOKENS, WIDE), lambda i, k: (4 * i + k, 0)),
            out_shape=jax.ShapeDtypeStruct((NARROW, WIDE), f32), **common)(gathered)
    return pl.pallas_call(
        functools.partial(place_in_kernel, False),
        in_specs=[pl.BlockSpec((1, 1, 4, 2, 1, TOKENS, WIDTH), lambda i, k: (k, i, 0, 0, index, 0, 0))],
        out_specs=pl.BlockSpec((TOKENS, WIDE), lambda i, k: (4 * i + k, 0)),
        out_shape=jax.ShapeDtypeStruct((NARROW, WIDE), f32), **common)(gathered)


def solution(mesh):
    def device_step(x_one, z_one, x_two, z_two, grad_out, w1_in, w1_out, w2_in, w2_out):
        early, late, grad_pre, dx_two = reduce_factors(
            gelu(z_two), gelu(z_one), z_two, z_one, grad_out, x_two, x_one,
            w2_out.reshape(64, TOKENS, NARROW), w2_in.reshape(16, TOKENS, WIDE), w1_out.reshape(64, TOKENS, NARROW))
        dz_one = grad_pre[1].transpose(1, 0, 2).reshape(TOKENS, WIDE)
        dx_one = (dx_two.astype(jnp.float32) + lax.dot_general(dz_one, w1_in, CONTRACT_COLS, preferred_element_type=jnp.float32)).astype(jnp.bfloat16)

        def gather(part):
            whole = lax.all_gather(part, AXES, axis=0)
            return whole.reshape(CHIPS, CHIPS, CHIPS, 2, part.shape[0], TOKENS, WIDTH)

        first = gather(early)
        held, first = lax.optimization_barrier((late, first))
        last = gather(held)
        return (place(first, 0, 0), place(first, 1, 1), place(first, 2, 2), place(last, 0, 3), dx_one)

    row_spec = P(AXES, None)
    repl_spec = P()
    return jax.shard_map(
        device_step, mesh=mesh,
        in_specs=(row_spec,) * 5 + (repl_spec,) * 4,
        out_specs=(repl_spec,) * 4 + (row_spec,),
        check_vma=False,
    )
```

```python
import functools
import math
import jax
import jax.numpy as jnp
from jax import lax
from jax.experimental import pallas as pl
from jax.experimental.pallas import tpu as pltpu
from jax.sharding import PartitionSpec as P

AXES = ('third', 'second', 'group')
MESH = pl.DeviceIdType.MESH
INV_ROOT_TWO = math.sqrt(0.5)
INV_ROOT_TWO_PI = 1.0 / math.sqrt(2.0 * math.pi)
CONTRACT_ROWS = (((0,), (0,)), ((), ()))
CONTRACT_COLS = (((1,), (1,)), ((), ()))
ROLES = (('x', 'y', 'z'), ('y', 'z', 'x'), ('z', 'x', 'y'), ('x', 'y', 'z'))
GATHER = ('yzx', 'zxy', 'xyz')
HALF = 512
CHIPS = 4
LINE = 8
TOKENS = 128
WIDTH = 1024
NARROW = 2048
WIDE = 8192
BOTH = (0, 1)
PAIR = 2
BACK = 3
COLOR_ROWS = 64
SLOTS = 6
ORDER = tuple(zip(map(int, '0102130451023410652317647523647523467567'), map(int, '0010102002311134012240121233232344433444')))


def gelu(z_pre):
    z_val = z_pre.astype(jnp.float32)
    return (z_val * (0.5 * (1.0 + lax.erf(z_val * INV_ROOT_TWO)))).astype(jnp.bfloat16)


def slope_of(z_pre):
    z_val = z_pre.astype(jnp.float32)
    cdf_val = 0.5 * (1.0 + lax.erf(z_val * INV_ROOT_TWO))
    return cdf_val + z_val * jnp.exp(-0.5 * z_val * z_val) * INV_ROOT_TWO_PI


def reduce_kernel(hid_two, hid_one, z_two, z_one, grad_out, x_two, x_one, w2_out, w2_in, w1_out,
                  ring_ref, own_ref, last_ref, dz_out, dx_two, land_w, land_n,
                  stage_w, stage_n, part, got1, got2, got3, got4, dz_buf, dy_buf, dx_buf, z_buf,
                  xs_n, xr_n, xs_w, xr_w, stage_sem_w, stage_sem_n, rs_send, rs_recv, z_sem, put_sem):
    narrows = (grad_out, x_two, dx_two, x_one)

    def wide_piece(m, line, h):
        if m % PAIR:
            return dz_out.at[m // PAIR, PAIR * line + h]
        return (hid_two, hid_one)[m // PAIR].at[:, pl.ds(pl.multiple_of(line * WIDTH + h * HALF, HALF), HALF)]

    def fetch_tile(which, t):
        slot = t % PAIR
        if which == 1:
            def columns(k, carry):
                pltpu.make_async_copy(w2_in.at[pl.ds(PAIR * t, PAIR), :, pl.ds(pl.multiple_of(k * NARROW, NARROW), NARROW)],
                                      stage_n.at[slot, pl.ds(PAIR * k, PAIR)], stage_sem_n.at[slot]).start()
                return carry
            lax.fori_loop(0, 4, columns, 0)
        else:
            pltpu.make_async_copy((w2_out, None, w1_out)[which].at[pl.ds(8 * t, 8)], stage_n.at[slot], stage_sem_n.at[slot]).start()
            z_pre = (z_two, None, z_one)[which]
            pltpu.make_async_copy(z_pre.at[:, pl.ds(pl.multiple_of(t * WIDTH, WIDTH), WIDTH)], z_buf.at[slot], z_sem.at[slot]).start()

    def tiles(which, body):
        def step(t, carry):
            slot = t % PAIR
            pltpu.make_async_copy(stage_n.at[slot], stage_n.at[slot], stage_sem_n.at[slot]).wait()
            if which != 1:
                pltpu.make_async_copy(z_buf.at[slot], z_buf.at[slot], z_sem.at[slot]).wait()
            body(t, slot)

            @pl.when(t < 6)
            def _():
                fetch_tile(which, t + PAIR)
            if which < PAIR:
                @pl.when(t >= 6)
                def _():
                    fetch_tile(which + 1, t - 6)
            return carry
        lax.fori_loop(0, 8, step, 0)

    def weights(slot, pair):
        return stage_n[slot, PAIR * pair:PAIR * pair + PAIR].reshape(256, NARROW)

    def grad_pre(which, grad_ref):
        def body(t, slot):
            for pair in range(4):
                grad_hidden = lax.dot_general(grad_ref[...], weights(slot, pair), CONTRACT_COLS, preferred_element_type=jnp.float32)
                at = 256 * (pair % PAIR)
                slope = slope_of(z_buf[slot, :, 256 * pair:256 * pair + 256])
                dz_buf[PAIR * t + pair // PAIR, :, at:at + 256] = (grad_hidden * slope).astype(jnp.bfloat16)
        tiles(which, body)
        put = pltpu.make_async_copy(dz_buf, dz_out.at[which // PAIR], put_sem.at[0])
        put.start()
        put.wait()

    def grad_input():
        def body(t, slot):
            total = None
            for k in range(16):
                at = HALF * (k % CHIPS)
                prod = lax.dot_general(dz_buf[k], weights(slot, k // 4)[:, at:at + HALF], CONTRACT_COLS, preferred_element_type=jnp.float32)
                total = prod if total is None else total + prod
            cols = pl.ds(pl.multiple_of(t * 256, 256), 256)
            dx_buf[:, cols] = (dy_buf[:, cols].astype(jnp.float32) + total).astype(jnp.bfloat16)
        tiles(1, body)
        put = pltpu.make_async_copy(dx_buf, dx_two, put_sem.at[1])
        put.start()
        put.wait()

    fetch_tile(0, 0)
    fetch_tile(0, 1)
    get_dy = pltpu.make_async_copy(grad_out, dy_buf, put_sem.at[1])
    get_dy.start()
    z, y, g = lax.axis_index('third'), lax.axis_index('second'), lax.axis_index('group')
    x, c = g // PAIR, g % PAIR
    pos = {'x': x, 'y': y, 'z': z}

    def device(axis, off, core):
        at = dict(pos)
        at[axis] = (pos[axis] + off) % CHIPS
        return (at['z'], at['y'], PAIR * at['x'] + core)

    barrier = pltpu.get_barrier_semaphore()
    peers = [device(axis, off, core) for axis in 'xyz' for off in (1, PAIR, BACK) for core in BOTH] + [device('x', 0, 1 - c)]
    for peer in peers:
        pl.semaphore_signal(barrier, inc=1, device_id=peer, device_id_type=MESH)
    pl.semaphore_wait(barrier, len(peers))

    def line_index(m):
        return PAIR * pos[ROLES[m][0]] + c

    def direct_narrow(m, off, core):
        return pltpu.make_async_remote_copy(
            src_ref=narrows[m], dst_ref=land_n.at[m, line_index(m)], send_sem=xs_n.at[m, off], recv_sem=xr_n.at[m, line_index(m)],
            device_id=device(ROLES[m][0], off, core), device_id_type=MESH)

    def relay_narrow(m, off):
        source = PAIR * ((pos[ROLES[m][0]] + off) % CHIPS) + c
        return pltpu.make_async_remote_copy(
            src_ref=land_n.at[m, source], dst_ref=land_n.at[m, source], send_sem=xs_n.at[m, BACK + off], recv_sem=xr_n.at[m, source],
            device_id=device('x', 0, 1 - c), device_id_type=MESH)

    def wide_copy(m, h, off, core):
        me = line_index(m)
        target = PAIR * ((pos[ROLES[m][0]] + off) % CHIPS) + core
        return pltpu.make_async_remote_copy(
            src_ref=wide_piece(m, target, h), dst_ref=land_w.at[m, h, me], send_sem=xs_w.at[m, h, PAIR * off + core], recv_sem=xr_w.at[m, h, me],
            device_id=device(ROLES[m][0], off, core), device_id_type=MESH)

    def over_chips(fn):
        lax.fori_loop(1, 4, lambda off, carry: (fn(off), carry)[1], 0)

    def start_narrow(m):
        over_chips(lambda off: direct_narrow(m, off, c).start())
        direct_narrow(m, 0, 1 - c).start()

    def start_wide(m, h):
        def both(off):
            wide_copy(m, h, off, 0).start()
            wide_copy(m, h, off, 1).start()
        over_chips(both)
        wide_copy(m, h, 0, 1 - c).start()

    def relay(m):
        def one(off):
            source = PAIR * ((pos[ROLES[m][0]] + off) % CHIPS) + c
            pltpu.make_async_copy(land_n.at[m, source], land_n.at[m, source], xr_n.at[m, source]).wait()
            relay_narrow(m, off).start()
        over_chips(one)

    def wait_exchange_sends(m):
        over_chips(lambda off: direct_narrow(m, off, c).wait_send())
        direct_narrow(m, 0, 1 - c).wait_send()
        over_chips(lambda off: relay_narrow(m, off).wait_send())
        for h in BOTH:
            def both(off):
                wide_copy(m, h, off, 0).wait_send()
                wide_copy(m, h, off, 1).wait_send()
            over_chips(both)
            wide_copy(m, h, 0, 1 - c).wait_send()

    def stage_narrow(m):
        me = line_index(m)
        slot = m % PAIR

        def other_core(off, carry):
            source = PAIR * ((pos[ROLES[m][0]] + off) % CHIPS) + 1 - c
            pltpu.make_async_copy(land_n.at[m, source], land_n.at[m, source], xr_n.at[m, source]).wait()
            return carry
        lax.fori_loop(0, 4, other_core, 0)

        def fetch(off, carry):
            source = (me + off) % LINE
            pltpu.make_async_copy(land_n.at[m, source], stage_n.at[slot, source], stage_sem_n.at[slot]).start()
            return carry
        lax.fori_loop(1, LINE, fetch, 0)
        pltpu.make_async_copy(narrows[m], stage_n.at[slot, me], stage_sem_n.at[slot]).start()

    def stage_wide(m, h):
        me = line_index(m)

        def fetch(off, carry):
            source = (me + off) % LINE
            pltpu.make_async_copy(land_w.at[m, h, source], land_w.at[m, h, source], xr_w.at[m, h, source]).wait()
            pltpu.make_async_copy(land_w.at[m, h, source], stage_w.at[h, source], stage_sem_w.at[h]).start()
            return carry
        lax.fori_loop(1, LINE, fetch, 0)
        pltpu.make_async_copy(wide_piece(m, me, h), stage_w.at[h, me], stage_sem_w.at[h]).start()

    def rs_copy(j, color, stage, side):
        m, h = j // PAIR, j % PAIR
        first, second = ROLES[m][1:] if color == 0 else ROLES[m][:0:-1]
        p, q = pos[first], pos[second]
        slot, got = j % SLOTS, j % 6
        sign = 1 if side == 0 else BACK
        mine = part.at[slot, color]
        if stage == 1:
            src, dst, axis = mine.at[(p + PAIR) % CHIPS, pl.ds(PAIR * side, PAIR)], got1.at[got, color, side], first
        elif stage == PAIR:
            src, dst, axis = mine.at[(p + sign) % CHIPS], got2.at[got, color, side], first
        elif stage == BACK:
            src, dst, axis = mine.at[p, (q + PAIR) % CHIPS, pl.ds(32 * side, 32)], got3.at[got, color, side], second
        else:
            src, dst, axis = mine.at[p, (q + sign) % CHIPS], got4.at[got, color, side], second
        return pltpu.make_async_remote_copy(
            src_ref=src, dst_ref=dst, send_sem=rs_send.at[j, color, stage - 1, side], recv_sem=rs_recv.at[j, color, stage - 1, side],
            device_id=device(axis, sign, c), device_id_type=MESH)

    def compute(j):
        m, h = j // PAIR, j % PAIR
        slot = j % SLOTS
        a, b = pos[ROLES[m][1]], pos[ROLES[m][PAIR]]
        if h == 0:
            pltpu.make_async_copy(stage_n.at[m % PAIR], stage_n.at[m % PAIR], stage_sem_n.at[m % PAIR]).wait()
        pltpu.make_async_copy(stage_w.at[h], stage_w.at[h], stage_sem_w.at[h]).wait()
        wide, narrow = stage_w.at[h], stage_n.at[m % PAIR]

        def piece(i, carry):
            k = jnp.maximum(i - 7, 0)
            pa = jnp.where(i < 4, a + PAIR, jnp.where(i < 7, a + i - 1, a + BACK + k // BACK)) % CHIPS
            pb = jnp.where(i < 4, i, jnp.where(i < 7, b + PAIR, b + BACK + k % BACK)) % CHIPS
            if m % PAIR == 0:
                lhs, lhs_at, rhs, rhs_at = wide, pa * TOKENS, narrow, pb * HALF
            else:
                lhs, lhs_at, rhs, rhs_at = narrow, (pa * 4 + pb) * TOKENS, wide, 0
            lhs_cols = pl.ds(pl.multiple_of(lhs_at, TOKENS), TOKENS)
            rhs_cols = pl.ds(pl.multiple_of(rhs_at, HALF), HALF) if m % PAIR == 0 else slice(None)
            total = None
            for dev in range(8):
                prod = lax.dot_general(lhs[dev, :, lhs_cols], rhs[dev, :, rhs_cols], CONTRACT_ROWS, preferred_element_type=jnp.float32)
                prod = prod.astype(jnp.bfloat16).astype(jnp.float32)
                total = prod if total is None else total + prod
            part[slot, 0, pa, pb] = total[:COLOR_ROWS]
            part[slot, 1, pb, pa] = total[COLOR_ROWS:]

            @pl.when(i == BACK)
            def _():
                rs_copy(j, 0, 1, 0).start()
                rs_copy(j, 0, 1, 1).start()

            @pl.when(i == 6)
            def _():
                rs_copy(j, 1, 1, 0).start()
                rs_copy(j, 1, 1, 1).start()
            return carry
        lax.fori_loop(0, 16, piece, 0)

    def coords(j, color):
        m = j // PAIR
        first, second = ROLES[m][1:] if color == 0 else ROLES[m][:0:-1]
        return pos[first], pos[second]

    def stage_two(j):
        slot, got = j % SLOTS, j % 6
        for color in BOTH:
            p, q = coords(j, color)
            rs_copy(j, color, 1, 0).wait_recv()
            part[slot, color, (p + 1) % CHIPS, 0:PAIR] += got1[got, color, 0]
            rs_copy(j, color, 1, 1).wait_recv()
            part[slot, color, (p + BACK) % CHIPS, PAIR:4] += got1[got, color, 1]
            rs_copy(j, color, PAIR, 0).start()
            rs_copy(j, color, PAIR, 1).start()

    def stage_three(j):
        slot, got = j % SLOTS, j % 6
        for color in BOTH:
            p, q = coords(j, color)
            rs_copy(j, color, PAIR, 0).wait_recv()
            rs_copy(j, color, PAIR, 1).wait_recv()
            part[slot, color, p] += got2[got, color, 0] + got2[got, color, 1]
        for color in BOTH:
            rs_copy(j, color, BACK, 0).start()
            rs_copy(j, color, BACK, 1).start()

    def stage_four(j):
        slot, got = j % SLOTS, j % 6
        for color in BOTH:
            p, q = coords(j, color)
            rs_copy(j, color, BACK, 0).wait_recv()
            part[slot, color, p, (q + 1) % CHIPS, 0:32] += got3[got, color, 0]
            rs_copy(j, color, BACK, 1).wait_recv()
            part[slot, color, p, (q + BACK) % CHIPS, 32:COLOR_ROWS] += got3[got, color, 1]
            rs_copy(j, color, 4, 0).start()
            rs_copy(j, color, 4, 1).start()

    def stage_five(j):
        m, h = j // PAIR, j % PAIR
        slot, got = j % SLOTS, j % 6
        for color in BOTH:
            p, q = coords(j, color)
            rs_copy(j, color, 4, 0).wait_recv()
            rs_copy(j, color, 4, 1).wait_recv()
            if m < PAIR:
                out_ref = ring_ref.at[m, pl.ds(COLOR_ROWS * color, COLOR_ROWS)]
            elif m == BACK:
                out_ref = own_ref.at[color]
            else:
                out_ref = last_ref.at[0] if color else own_ref.at[PAIR]
            out_ref[:, h * HALF:(h + 1) * HALF] = part[slot, color, p, q] + got4[got, color, 0] + got4[got, color, 1]

    def drain(j):
        for color in BOTH:
            for stage in (1, PAIR, BACK, 4):
                for side in BOTH:
                    rs_copy(j, color, stage, side).wait_send()

    start_narrow(0)
    start_narrow(1)
    for h in BOTH:
        start_wide(0, h)
    for h in BOTH:
        start_wide(PAIR, h)
    start_narrow(BACK)
    get_dy.wait()
    grad_pre(0, dy_buf)
    for h in BOTH:
        start_wide(1, h)
    grad_input()
    start_narrow(PAIR)
    relay(0)
    relay(1)
    grad_pre(PAIR, dx_buf)
    for h in BOTH:
        start_wide(BACK, h)
    stage_narrow(0)
    stage_wide(0, 0)

    def compute_step(j):
        if j == 6:
            relay(BACK)
            stage_narrow(BACK)
            stage_wide(BACK, 0)
        if j >= SLOTS:
            drain(j - SLOTS)
        if j + 1 < 8 and j + 1 != 6:
            if j + 1 == 4:
                relay(PAIR)
            if (j + 1) % PAIR == 0:
                stage_narrow((j + 1) // PAIR)
            stage_wide((j + 1) // PAIR, (j + 1) % PAIR)
        compute(j)

    steps = (compute_step, stage_two, stage_three, stage_four, stage_five)
    for job, stage in ORDER:
        steps[stage](job)
    for j in range(8 - SLOTS, 8):
        drain(j)
    for m in range(4):
        wait_exchange_sends(m)


def reduce_factors(*operands):
    f32, bf16, dma = jnp.float32, jnp.bfloat16, pltpu.SemaphoreType.DMA
    any_spec = pl.BlockSpec(memory_space=pl.ANY)
    vmem_spec = pl.BlockSpec(memory_space=pltpu.VMEM)
    return pl.pallas_call(
        reduce_kernel,
        out_shape=(jax.ShapeDtypeStruct((PAIR, TOKENS, WIDTH), f32), jax.ShapeDtypeStruct((BACK, COLOR_ROWS, WIDTH), f32), jax.ShapeDtypeStruct((1, COLOR_ROWS, WIDTH), f32),
                   jax.ShapeDtypeStruct((PAIR, 16, TOKENS, HALF), bf16), jax.ShapeDtypeStruct((TOKENS, NARROW), bf16),
                   jax.ShapeDtypeStruct((4, PAIR, 8, TOKENS, HALF), bf16), jax.ShapeDtypeStruct((4, 8, TOKENS, NARROW), bf16)),
        in_specs=[any_spec] * len(operands),
        out_specs=(vmem_spec,) * BACK + (any_spec,) * 4,
        scratch_shapes=[
            pltpu.VMEM((PAIR, 8, TOKENS, HALF), bf16), pltpu.VMEM((PAIR, 8, TOKENS, NARROW), bf16),
            pltpu.VMEM((SLOTS, PAIR, 4, 4, COLOR_ROWS, HALF), f32),
            pltpu.VMEM((6, PAIR, PAIR, PAIR, COLOR_ROWS, HALF), f32), pltpu.VMEM((6, PAIR, PAIR, 4, COLOR_ROWS, HALF), f32),
            pltpu.VMEM((6, PAIR, PAIR, 32, HALF), f32), pltpu.VMEM((6, PAIR, PAIR, COLOR_ROWS, HALF), f32),
            pltpu.VMEM((16, TOKENS, HALF), bf16), pltpu.VMEM((TOKENS, NARROW), bf16), pltpu.VMEM((TOKENS, NARROW), bf16), pltpu.VMEM((PAIR, TOKENS, WIDTH), bf16),
            dma((4, 8)), dma((4, 8)), dma((4, PAIR, 8)), dma((4, PAIR, 8)), dma((PAIR,)), dma((PAIR,)),
            dma((8, PAIR, 4, PAIR)), dma((8, PAIR, 4, PAIR)), dma((PAIR,)), dma((PAIR,)),
        ],
        compiler_params=pltpu.CompilerParams(collective_id=0, has_side_effects=True, vmem_limit_bytes=67043328),
        cost_estimate=pl.CostEstimate(flops=1 << 34, bytes_accessed=COLOR_ROWS << 20, transcendentals=0),
        name='reduce_factors',
    )(*operands)[:5]


def gather_kernel(own_ref, whole0, whole1, whole2, held, get_sem, put_sem, send_sem, recv_sem):
    wholes = (whole0, whole1, whole2)
    z, y, g = lax.axis_index('third'), lax.axis_index('second'), lax.axis_index('group')
    x, c = g // PAIR, g % PAIR
    pos = {'x': x, 'y': y, 'z': z}

    def device(axis, off, core):
        at = dict(pos)
        at[axis] = (pos[axis] + off) % CHIPS
        return (at['z'], at['y'], PAIR * at['x'] + core)

    gets = [pltpu.make_async_copy(own_ref.at[i], held.at[i], get_sem.at[i]) for i in range(BACK)]
    for get in gets:
        get.start()
    barrier = pltpu.get_barrier_semaphore()
    peers = [device(axis, off, c) for axis in 'xyz' for off in (1, BACK)] + [device('x', 0, 1 - c)]
    for peer in peers:
        pl.semaphore_signal(barrier, inc=1, device_id=peer, device_id_type=MESH)
    pl.semaphore_wait(barrier, len(peers))

    def copy(i, n):
        axes = GATHER[i]
        p1, p2, p3 = [pos[axis] for axis in axes]
        mine = wholes[i].at[c]
        side = n % PAIR
        back = BACK - PAIR * side
        rows = (p2, (p2 + BACK) % CHIPS, (p2 + 1) % CHIPS, (p2 + PAIR) % CHIPS)
        src = None
        axis, off = axes[0], 1 + PAIR * side
        if n < PAIR:
            dst, src = mine.at[p3, p2, p1], held.at[i]
        elif n < 4:
            dst = mine.at[p3, p2, (p1 + back) % CHIPS, pl.ds(32 * side, 32)]
        elif n < 6:
            axis, dst = axes[1], mine.at[p3, p2]
        elif n < 8:
            axis, dst = axes[1], mine.at[p3, (p2 + back) % CHIPS, pl.ds(PAIR * side, PAIR)]
        elif n < 16:
            axis, dst = axes[PAIR], mine.at[p3, rows[(n - 8) // PAIR]]
        elif n < 20:
            axis, dst = axes[PAIR], mine.at[(p3 + back) % CHIPS, rows[PAIR * side + (n - 16) // PAIR]]
        else:
            axis, off, dst = axes[PAIR], 0, mine.at[(p3, (p3 + BACK) % CHIPS, (p3 + 1) % CHIPS, (p3 + PAIR) % CHIPS)[(n - 20) // 4], rows[n % CHIPS]]
        return pltpu.make_async_remote_copy(
            src_ref=dst if src is None else src, dst_ref=dst, send_sem=send_sem.at[i, n], recv_sem=recv_sem.at[i, n],
            device_id=device(axis, off, c if n < 20 else 1 - c), device_id_type=MESH)

    def start(i, *which):
        for n in which:
            copy(i, n).start()

    def wait(i, *which):
        for n in which:
            copy(i, n).wait_recv()

    puts = []
    for i in range(BACK):
        p1, p2, p3 = [pos[axis] for axis in GATHER[i]]
        gets[i].wait()
        start(i, 0, 1)
        puts.append(pltpu.make_async_copy(held.at[i], wholes[i].at[c, p3, p2, p1], put_sem.at[i]))
        puts[i].start()
    for i in range(BACK):
        for side in BOTH:
            wait(i, side)
            start(i, PAIR + side)
    for i in range(BACK):
        puts[i].wait()
        wait(i, PAIR, BACK)
        start(i, 4, 5, 20)
    for i in range(BACK):
        for side in BOTH:
            wait(i, 4 + side)
            start(i, 6 + side)
    for k in range(BACK):
        for i in range(BACK):
            start(i, 8 + PAIR * k, 9 + PAIR * k)
            if k:
                start(i, 20 + k)
    for i in range(BACK):
        wait(i, 6, 7)
        start(i, 14, 15, 23)
    for k in range(4):
        for i in range(BACK):
            for side in BOTH:
                wait(i, 8 + PAIR * k + side)
                if k // PAIR == side:
                    start(i, 16 + PAIR * (k % PAIR) + side)
                start(i, 24 + 4 * side + k)
    for k in range(PAIR):
        for i in range(BACK):
            for side in BOTH:
                wait(i, 16 + PAIR * k + side)
                start(i, 32 + PAIR * side + k)
    for i in range(BACK):
        wait(i, *range(20, 36))
        for n in range(36):
            copy(i, n).wait_send()


def gather_own(own):
    f32, dma = jnp.float32, pltpu.SemaphoreType.DMA
    any_spec = pl.BlockSpec(memory_space=pl.ANY)
    return pl.pallas_call(
        gather_kernel,
        out_shape=(jax.ShapeDtypeStruct((PAIR, 4, 4, 4, COLOR_ROWS, WIDTH), f32),) * BACK,
        in_specs=[any_spec],
        out_specs=(any_spec,) * BACK,
        scratch_shapes=[pltpu.VMEM((BACK, COLOR_ROWS, WIDTH), f32), dma((BACK,)), dma((BACK,)), dma((BACK, 36)), dma((BACK, 36))],
        compiler_params=pltpu.CompilerParams(collective_id=1, has_side_effects=True),
        cost_estimate=pl.CostEstimate(flops=1 << 38, bytes_accessed=96 << 20, transcendentals=0),
        name='gather_own',
    )(own)


def columns_kernel(pick, in_ref, *rest):
    out_ref = rest[-1]
    for q in range(4):
        for line in range(out_ref.shape[0]):
            for h in BOTH:
                out_ref[line, h, 0, :, q * HALF:(q + 1) * HALF] = in_ref[pick(q, line)][:, h * HALF:(h + 1) * HALF]


def rows_kernel(picks, *refs):
    out_ref = refs[-1]
    for e in range(4):
        for core in BOTH:
            at = (PAIR * e + core) * WIDTH
            for pick, in_ref in zip(picks, refs):
                piece = in_ref[pick(e, core)]
                first = len(piece) * picks.index(pick)
                out_ref[first:first + len(piece), at:at + WIDTH] = piece


def place(kernel, grid, blocks, arrays, out_shape, out_block, out_index, into=None):
    in_specs = [pl.BlockSpec(block, index) for block, index in blocks]
    if into is not None:
        in_specs.append(pl.BlockSpec(memory_space=pl.ANY))
        arrays = arrays + (into,)
    return pl.pallas_call(
        kernel, grid=grid, in_specs=in_specs, out_specs=pl.BlockSpec(out_block, out_index),
        out_shape=jax.ShapeDtypeStruct(out_shape, jnp.float32),
        input_output_aliases={} if into is None else {len(in_specs) - 1: 0},
        cost_estimate=pl.CostEstimate(flops=1 << 30, bytes_accessed=TOKENS << 20, transcendentals=0), name='place',
    )(*arrays)


OUT_SHAPE = (8, PAIR, 4, TOKENS, NARROW)


def place_zero(ring):
    return place(functools.partial(columns_kernel, lambda q, line: (q, 0, 0, line, 0)), (4, 4),
                 [((4, 1, 1, PAIR, 1, TOKENS, WIDTH), lambda i, k: (0, i, k, 0, 0, 0, 0))], (ring,),
                 OUT_SHAPE, (PAIR, PAIR, 1, TOKENS, NARROW), lambda i, k: (k, 0, i, 0, 0)).reshape(WIDE, NARROW)


def place_one(ring):
    return place(functools.partial(rows_kernel, (lambda e, core: (0, e, 0, core, 0),)), (4, 4),
                 [((1, 4, 1, PAIR, 1, TOKENS, WIDTH), lambda i, k: (i, 0, k, 0, 1, 0, 0))], (ring,),
                 (NARROW, WIDE), (TOKENS, WIDE), lambda i, k: (4 * i + k, 0))


def place_two_low(piece):
    return place(functools.partial(columns_kernel, lambda q, line: (line % PAIR, line // PAIR, q, 0)), (4, PAIR),
                 [((PAIR, PAIR, 4, 1, COLOR_ROWS, WIDTH), lambda i, k: (0, k, 0, i, 0, 0))], (piece,),
                 OUT_SHAPE, (4, PAIR, 1, COLOR_ROWS, NARROW), lambda i, k: (k, 0, i, 0, 0))


def place_two_high(ring, low):
    return place(functools.partial(columns_kernel, lambda q, line: (line // PAIR, q, 0, line % PAIR, 0)), (4, PAIR),
                 [((PAIR, 4, 1, PAIR, 1, COLOR_ROWS, WIDTH), lambda i, k: (k, 0, i, 0, 0, 0, 0))], (ring,),
                 OUT_SHAPE, (4, PAIR, 1, COLOR_ROWS, NARROW), lambda i, k: (k, 0, i, 1, 0), low).reshape(WIDE, NARROW)


def place_three(low, high):
    return place(functools.partial(rows_kernel, (lambda e, core: (core, e, 0, 0), lambda e, core: (core, 0, e, 0))), (4, 4),
                 [((PAIR, 4, 1, 1, COLOR_ROWS, WIDTH), lambda i, k: (0, 0, k, i, 0, 0)), ((PAIR, 1, 4, 1, COLOR_ROWS, WIDTH), lambda i, k: (0, i, 0, k, 0, 0))],
                 (low, high), (NARROW, WIDE), (TOKENS, WIDE), lambda i, k: (4 * i + k, 0))


def solution(mesh):
    def device_step(x_one, z_one, x_two, z_two, grad_out, w1_in, w1_out, w2_in, w2_out):
        ring, own, last, grad_pre, dx_two = reduce_factors(
            gelu(z_two), gelu(z_one), z_two, z_one, grad_out, x_two, x_one,
            w2_out.reshape(COLOR_ROWS, TOKENS, NARROW), w2_in.reshape(16, TOKENS, WIDE), w1_out.reshape(COLOR_ROWS, TOKENS, NARROW))
        dz_one = grad_pre[1].transpose(1, 0, PAIR).reshape(TOKENS, WIDE)
        dx_one = (dx_two.astype(jnp.float32) + lax.dot_general(dz_one, w1_in, CONTRACT_COLS, preferred_element_type=jnp.float32)).astype(jnp.bfloat16)

        def gather(part):
            whole = lax.all_gather(part, AXES, axis=0)
            return whole.reshape(CHIPS, CHIPS, CHIPS, PAIR, *part.shape)

        first = gather(ring)
        three_low, three_high, two_low = gather_own(own)
        sum_three = place_three(three_low, three_high)
        sum_two = place_two_low(two_low)
        last, first, sum_two, sum_three = lax.optimization_barrier((last, first, sum_two, sum_three))
        sum_two = place_two_high(gather(last), sum_two)
        return (place_zero(first), place_one(first), sum_two, sum_three, dx_one)

    row_spec = P(AXES, None)
    repl_spec = P()
    return jax.shard_map(
        device_step, mesh=mesh,
        in_specs=(row_spec,) * 5 + (repl_spec,) * 4,
        out_specs=(repl_spec,) * 4 + (row_spec,),
        check_vma=False,
    )
```
